32 devices in a mesh: dp: 2 (over core), fsdp: 16 (over z, y, x).
Axes of the slice: x: 2, y: 2, z: 4, core: 2. Of those that a mesh axis runs over, the one named last changes fastest.
Arguments:
- tokens: bfloat16 [2, 32, 576, 768], P(None, ('dp', 'fsdp')), may hold values from -6 to 6
- near_bucket: int32 [2, 32, 576, 576], P(None, ('dp', 'fsdp')), may hold values from 0 to 31
- x_bucket: int32 [2, 32, 576, 576], P(None, ('dp', 'fsdp')), may hold values from 0 to 63
- y_bucket: int32 [2, 32, 576, 576], P(None, ('dp', 'fsdp')), may hold values from 0 to 63
- key_mask: int32 [2, 32, 576], P(None, ('dp', 'fsdp')), may hold values 0 or 1
- out_grad: bfloat16 [2, 32, 576, 768], P(None, ('dp', 'fsdp')), may hold values from -6 to 6
- w_query: bfloat16 [768, 768], P(('dp', 'fsdp')), may hold values from -0.21875 to 0.21875
- w_key: bfloat16 [768, 768], P(('dp', 'fsdp')), may hold values from -0.21875 to 0.21875
- w_value: bfloat16 [768, 768], P(('dp', 'fsdp')), may hold values from -0.21875 to 0.21875
- w_out: bfloat16 [768, 768], P(('dp', 'fsdp')), may hold values from -1.75 to 1.75
- w_up: bfloat16 [768, 3072], P(('dp', 'fsdp')), may hold values from -0.21875 to 0.21875
- w_down: bfloat16 [3072, 768], P(('dp', 'fsdp')), may hold values from -0.109375 to 0.109375
- b_query: bfloat16 [768], P(('dp', 'fsdp')), may hold values from -3 to 3
- b_value: bfloat16 [768], P(('dp', 'fsdp')), may hold values from -3 to 3
- b_out: bfloat16 [768], P(('dp', 'fsdp')), may hold values from -3 to 3
- gain_first: bfloat16 [768], P(('dp', 'fsdp')), may hold values from 0.099609375 to 1.8984375
- shift_first: bfloat16 [768], P(('dp', 'fsdp')), may hold values from -3 to 3
- b_up: bfloat16 [3072], P(('dp', 'fsdp')), may hold values from -3 to 3
- b_down: bfloat16 [768], P(('dp', 'fsdp')), may hold values from -3 to 3
- gain_second: bfloat16 [768], P(('dp', 'fsdp')), may hold values from 0.099609375 to 1.8984375
- shift_second: bfloat16 [768], P(('dp', 'fsdp')), may hold values from -3 to 3
- table_near: bfloat16 [32, 12], P('fsdp'), may hold values from -6 to 6
- table_x: bfloat16 [64, 12], P('fsdp'), may hold values from -6 to 6
- table_y: bfloat16 [64, 12], P('fsdp'), may hold values from -6 to 6
Outputs:
- layer_out: bfloat16 [2, 32, 576, 768], P(None, ('dp', 'fsdp'))
- grad_tokens: bfloat16 [2, 32, 576, 768], P(None, ('dp', 'fsdp'))
- grad_w_query: float32 [768, 768], P(('dp', 'fsdp'))
- grad_w_key: float32 [768, 768], P(('dp', 'fsdp'))
- grad_w_value: float32 [768, 768], P(('dp', 'fsdp'))
- grad_w_out: float32 [768, 768], P(('dp', 'fsdp'))
- grad_w_up: float32 [768, 3072], P(('dp', 'fsdp'))
- grad_w_down: float32 [3072, 768], P(('dp', 'fsdp'))
- grad_b_query: float32 [768], P(('dp', 'fsdp'))
- grad_b_value: float32 [768], P(('dp', 'fsdp'))
- grad_b_out: float32 [768], P(('dp', 'fsdp'))
- grad_gain_first: float32 [768], P(('dp', 'fsdp'))
- grad_shift_first: float32 [768], P(('dp', 'fsdp'))
- grad_b_up: float32 [3072], P(('dp', 'fsdp'))
- grad_b_down: float32 [768], P(('dp', 'fsdp'))
- grad_gain_second: float32 [768], P(('dp', 'fsdp'))
- grad_shift_second: float32 [768], P(('dp', 'fsdp'))
- grad_table_near: float32 [32, 12], P('fsdp')
- grad_table_x: float32 [64, 12], P('fsdp')
- grad_table_y: float32 [64, 12], P('fsdp')
The draws below stay inside these ranges and needn't reach their ends.
All inputs are finite; a program needn't handle non-finite values. No bound on the sum of `key_mask` on one device may be relied on, other than what follows from the above.
Results may differ from the reference program's by a relative error of at most 0.015.
Values may be sent and summed in bfloat16 or wider, within the bound.
A program may use at most 384 MiB of HBM per device.

```python
import jax
import jax.numpy as jnp
from jax import lax

D = 768
H = 12
HD = 64
FF = 3072
NB1 = 32
NB2 = 64
L = 576
MICRO = 2
PAGES = 32


def with_ends(drawn, stream_key, low, top_value):
    place = [jax.random.randint(jax.random.fold_in(stream_key, axis), (), 0, length) for axis, length in enumerate(drawn.shape)]
    main_axis = drawn.shape.index(max(drawn.shape))
    neighbour = place[:main_axis] + [(place[main_axis] + 1) % drawn.shape[main_axis]] + place[main_axis + 1:]
    return drawn.at[tuple(place)].set(low).at[tuple(neighbour)].set(top_value)


def strengthened(array, rng, source, target, shards_of, factor):
    owner, partner = [(jnp.arange(array.shape[axis_at]) // (array.shape[axis_at] // shards_of)).reshape([-1 if axis == axis_at else 1 for axis in range(array.ndim)]) for axis_at in (source, target)]
    chosen = jax.random.permutation(rng, shards_of)[partner]
    strong = (owner == chosen) | (owner == (partner + shards_of // 2) % shards_of)
    return jnp.where(strong, factor * array, array)


def shard_levels(rng, dims, split, least, top_value):
    level = 1.0
    for axis_at, shards_of in split:
        draws = jax.random.uniform(jax.random.fold_in(jax.random.fold_in(rng, 6), axis_at), (shards_of,), jnp.float32, least / len(split), top_value / len(split))
        level = level * jnp.repeat(jnp.exp(draws), dims[axis_at] // shards_of).reshape((-1,) + (1,) * (len(dims) - 1 - axis_at))
    return level


def scatter_about(own_key, dims, spread, bound, split=(), held_as=jnp.bfloat16):
    drawn = spread * jax.random.normal(own_key, dims, jnp.float32)
    if split:
        drawn = drawn * shard_levels(own_key, dims, split, -0.22, 0.18)
    return jnp.clip(drawn, -bound, bound).astype(held_as)


def heavy_noise(own_key, shape, spread, most, split, heavy, kind=jnp.bfloat16):
    array = spread * jax.random.normal(own_key, shape, jnp.float32)
    if split:
        array = array * shard_levels(own_key, shape, split, -0.22, 0.18)
    return jnp.clip(strengthened(array, jax.random.fold_in(own_key, 3), *heavy), -most, most).astype(kind)


def setup_inputs(seed: int = 0) -> dict:
    key_of = jax.random.split(jax.random.key(seed), 25)
    return {
        "tokens": heavy_noise(key_of[0], (MICRO, PAGES, L, D), 1.0, 6.0, ((1, 32),), (1, 3, 32, 2.75)),
        "near_bucket": with_ends(jax.random.randint(key_of[1], (MICRO, PAGES, L, L), 0, NB1), jax.random.fold_in(key_of[1], 1), 0, NB1 - 1).astype(jnp.int32),
        "x_bucket": with_ends(jax.random.randint(key_of[2], (MICRO, PAGES, L, L), 0, NB2), jax.random.fold_in(key_of[2], 1), 0, NB2 - 1).astype(jnp.int32),
        "y_bucket": with_ends(jax.random.randint(key_of[3], (MICRO, PAGES, L, L), 0, NB2), jax.random.fold_in(key_of[3], 1), 0, NB2 - 1).astype(jnp.int32),
        "key_mask": with_ends((jax.random.randint(key_of[4], (MICRO, PAGES, L), 0, 8) < 7).astype(jnp.int32), jax.random.fold_in(key_of[4], 1), 0, 1),
        "out_grad": scatter_about(key_of[5], (MICRO, PAGES, L, D), 1.0, 6.0, ((1, 32),)),
        "w_query": scatter_about(key_of[6], (D, D), D ** -0.5, 0.21875, ((0, 32),)),
        "w_key": scatter_about(key_of[7], (D, D), D ** -0.5, 0.21875, ((0, 32),)),
        "w_value": scatter_about(key_of[8], (D, D), D ** -0.5, 0.21875, ((0, 32),)),
        "w_out": scatter_about(key_of[9], (D, D), (D // 64) ** -0.5, 1.75, ((0, 32),)),
        "w_up": scatter_about(key_of[10], (D, FF), D ** -0.5, 0.21875, ((0, 32),)),
        "w_down": scatter_about(key_of[11], (FF, D), FF ** -0.5, 0.109375, ((0, 32),)),
        "b_query": scatter_about(key_of[12], (D,), 0.5, 3.0, ((0, 32),)),
        "b_value": scatter_about(key_of[13], (D,), 0.5, 3.0, ((0, 32),)),
        "b_out": scatter_about(key_of[14], (D,), 0.5, 3.0, ((0, 32),)),
        "gain_first": jnp.clip(1.0 + 0.18 * jax.random.normal(key_of[15], (D,), jnp.float32), 0.099609375, 1.8984375).astype(jnp.bfloat16),
        "shift_first": scatter_about(key_of[16], (D,), 0.5, 3.0, ((0, 32),)),
        "b_up": scatter_about(key_of[17], (FF,), 0.5, 3.0, ((0, 32),)),
        "b_down": scatter_about(key_of[18], (D,), 0.5, 3.0, ((0, 32),)),
        "gain_second": jnp.clip(1.0 + 0.18 * jax.random.normal(key_of[19], (D,), jnp.float32), 0.099609375, 1.8984375).astype(jnp.bfloat16),
        "shift_second": scatter_about(key_of[20], (D,), 0.5, 3.0, ((0, 32),)),
        "table_near": scatter_about(key_of[21], (NB1, H), 1.0, 6.0, ((0, 16),)),
        "table_x": scatter_about(key_of[22], (NB2, H), 1.0, 6.0, ((0, 16),)),
        "table_y": scatter_about(key_of[23], (NB2, H), 1.0, 6.0, ((0, 16),)),
    }


@jax.custom_vjp
def low(v):
    return lax.optimization_barrier(v.astype(jnp.bfloat16)).astype(jnp.float32)

@jax.custom_vjp
def low_back(v):
    return v

def low_keep(v):
    return (low(v), None)

def low_pass(kept, grad):
    return (grad,)

def back_keep(v):
    return (v, None)

def back_low(kept, grad):
    return (low(grad),)
low.defvjp(low_keep, low_pass)
low_back.defvjp(back_keep, back_low)

def product(left_side, right_side):
    return jnp.dot(left_side, right_side, precision=lax.Precision.HIGHEST)

def layer_norm(inputs, gain_vec, shift_vec):
    average = lax.optimization_barrier(jnp.mean(inputs, axis=-1, keepdims=True))
    center = inputs - average
    spread_sq = lax.optimization_barrier(jnp.mean(center * center, axis=-1, keepdims=True))
    return center * lax.rsqrt(spread_sq + 1e-05) * gain_vec + shift_vec

def page_forward(params, tables, tokens, near_ids, x_ids, y_ids, allowed):
    w_query, w_key, w_value, w_out, w_up, w_down, b_query, b_value, b_out, gain_first, shift_first, b_up, b_down, gain_second, shift_second = params
    table_near, table_x, table_y = tables
    queries = low_back(low(product(tokens, w_query) + b_query)).reshape(L, H, HD)
    key_rows = low_back(low(product(tokens, w_key))).reshape(L, H, HD)
    values = low_back(low(product(tokens, w_value) + b_value)).reshape(L, H, HD)
    logits = jnp.einsum('lhe,mhe->hlm', queries, key_rows, precision=lax.Precision.HIGHEST) * 0.125
    rel_bias = jnp.transpose(table_near[near_ids] + table_x[x_ids] + table_y[y_ids], (2, 0, 1))
    scores = low_back(logits + rel_bias)
    scores = jnp.where(allowed[None], scores, -1e+30)
    attn_probs = low(jax.nn.softmax(scores, axis=-1))
    context = jnp.einsum('hlm,mhe->lhe', attn_probs, values, precision=lax.Precision.HIGHEST).reshape(L, D)
    context = low_back(low(context))
    branch_attn = low_back(product(context, w_out) + b_out)
    normed_one = layer_norm(tokens + branch_attn, gain_first, shift_first)
    hidden_pre = low_back(product(low(normed_one), w_up) + b_up)
    hidden = low(jax.nn.gelu(hidden_pre, approximate=False))
    branch_ffn = low_back(product(hidden, w_down) + b_down)
    return layer_norm(normed_one + branch_ffn, gain_second, shift_second)

def reference(tokens, near_bucket, x_bucket, y_bucket, key_mask, out_grad, w_query, w_key, w_value, w_out, w_up, w_down, b_query, b_value, b_out, gain_first, shift_first, b_up, b_down, gain_second, shift_second, table_near, table_x, table_y):
    params = tuple((entry.astype(jnp.float32) for entry in (w_query, w_key, w_value, w_out, w_up, w_down, b_query, b_value, b_out, gain_first, shift_first, b_up, b_down, gain_second, shift_second)))
    tables = (table_near.astype(jnp.float32), table_x.astype(jnp.float32), table_y.astype(jnp.float32))
    page_total = MICRO * PAGES
    page_items = (tokens.reshape(page_total, L, D), near_bucket.reshape(page_total, L, L), x_bucket.reshape(page_total, L, L), y_bucket.reshape(page_total, L, L), key_mask.reshape(page_total, L), out_grad.reshape(page_total, L, D))
    diagonal = jnp.arange(L)[:, None] == jnp.arange(L)[None, :]

    def page_step(running, page_item):
        page_tokens, near_ids, x_ids, y_ids, mask_row, cotangent = page_item
        allowed = (mask_row[None, :] > 0) | diagonal

        def closed(param_set, table_set, inputs):
            return page_forward(param_set, table_set, inputs, near_ids, x_ids, y_ids, allowed)
        result, pullback = jax.vjp(closed, params, tables, page_tokens.astype(jnp.float32))
        grad_params, grad_tables, grad_inputs = pullback(cotangent.astype(jnp.float32))
        running = jax.tree.map(lambda summed, latest: summed + latest, running, (grad_params, grad_tables))
        return (running, (result.astype(jnp.bfloat16), grad_inputs.astype(jnp.bfloat16)))
    initial = jax.tree.map(jnp.zeros_like, (params, tables))
    (grad_params, grad_tables), (outputs, input_grads) = lax.scan(page_step, initial, page_items)
    layer_out = outputs.reshape(MICRO, PAGES, L, D)
    grad_tokens = input_grads.reshape(MICRO, PAGES, L, D)
    return (layer_out, grad_tokens, grad_params[0], grad_params[1], grad_params[2], grad_params[3], grad_params[4], grad_params[5], grad_params[6], grad_params[7], grad_params[8], grad_params[9], grad_params[10], grad_params[11], grad_params[12], grad_params[13], grad_params[14], grad_tables[0], grad_tables[1], grad_tables[2])
```

```python
import functools
import jax
import jax.numpy as jnp
from jax import lax
from jax.experimental import pallas as pl
from jax.experimental.pallas import tpu as pltpu
from jax.sharding import PartitionSpec as P

BF, F32 = jnp.bfloat16, jnp.float32
NN = (((1,), (0,)), ((), ()))
NT = (((1,), (1,)), ((), ()))
TN = (((0,), (0,)), ((), ()))


def mm(left, right, dims=NN):
    return lax.dot_general(left, right, dims, preferred_element_type=F32)


def bias_kernel(near_ref, x_ref, y_ref, mask_ref, tab_ref, out_ref, *, heads, length):
    rows = near_ref.shape[1]
    base = pl.program_id(1) * rows

    def group(r, carry):
        start = pl.multiple_of(r * 8, 8)
        for lane in range(0, length, 128):
            width = min(128, length - lane)
            ids = []
            line = base + start + lax.broadcasted_iota(jnp.int32, (8, width), 0)
            column = lane + lax.broadcasted_iota(jnp.int32, (8, width), 1)
            allowed = (mask_ref[0, :, lane : lane + width] > 0) | (line == column)
            for which, ref in enumerate((near_ref, x_ref, y_ref)):
                part = ref[0, pl.ds(start, 8), lane : lane + width]
                if which == 0:
                    part = jnp.where(allowed, part, 127)
                if width < 128:
                    part = jnp.concatenate([part, jnp.zeros((8, 128 - width), jnp.int32)], axis=1)
                ids.append(part)
            sums = [None] * heads
            for which in range(3):
                for h in range(heads):
                    row = jnp.broadcast_to(tab_ref[which, h : h + 1, :], (8, 128))
                    got = jnp.take_along_axis(row, ids[which], axis=1)
                    sums[h] = got if which == 0 else sums[h] + got
            for h in range(heads):
                out_ref[0, h, pl.ds(start, 8), lane : lane + width] = sums[h][:, :width]
        return carry

    lax.fori_loop(0, rows // 8, group, 0)


def relative_bias(near, xb, yb, mask, tabs, rows=96):
    pages, length, _ = near.shape
    heads = tabs.shape[1]
    idx = pl.BlockSpec((1, rows, length), lambda p, r: (p, r, 0))
    return pl.pallas_call(
        functools.partial(bias_kernel, heads=heads, length=length),
        grid=(pages, length // rows),
        in_specs=[idx, idx, idx, pl.BlockSpec((1, 1, length), lambda p, r: (p, 0, 0)),
                  pl.BlockSpec((3, heads, 128), lambda p, r: (0, 0, 0))],
        out_specs=pl.BlockSpec((1, heads, rows, length), lambda p, r: (p, 0, r, 0)),
        out_shape=jax.ShapeDtypeStruct((pages, heads, length, length), F32),
        name="bias",
        cost_estimate=pl.CostEstimate(flops=30_000_000, bytes_accessed=60_000_000, transcendentals=0),
    )(near, xb, yb, mask, tabs)


def fwd_kernel(q_ref, k_ref, v_ref, bias_ref, e_ref, ctx_ref, inv_ref, *, rows):
    length = q_ref.shape[0]
    low_half = lax.broadcasted_iota(jnp.int32, (1, 128), 1) < 64
    keys = k_ref[...]
    values = v_ref[...]
    zero, one = jnp.zeros((), BF), jnp.ones((), BF)
    v_ext = (jnp.where(low_half, values, one), jnp.where(low_half, one, values))

    def chunk(c, carry):
        at = pl.ds(pl.multiple_of(c * rows, rows), rows)
        q = q_ref[at, :]
        q_sel = (jnp.where(low_half, q, zero), jnp.where(low_half, zero, q))
        outs = []
        for j in range(2):
            s = mm(q_sel[j], keys, NT) + bias_ref[0, j, at, :]
            e = jnp.exp(s - jnp.max(s, axis=1, keepdims=True)).astype(BF)
            e_ref[0, j, at, :] = e
            outs.append(mm(e, v_ext[j]))
        total = pltpu.roll(jnp.where(low_half, outs[1], outs[0]), 64, 1)
        inv = 1.0 / total
        inv_ref[at, :] = inv
        ctx_ref[at, :] = jnp.where(low_half, outs[0], outs[1]) * inv
        return carry

    lax.fori_loop(0, length // rows, chunk, 0)


def attention_fwd(q, k, v, bias, rows=96):
    pages, heads, length, _ = bias.shape
    feat = q.shape[1]
    tok = pl.BlockSpec((length, 128), lambda p, h: (p, h))
    mat = pl.BlockSpec((1, 2, length, length), lambda p, h: (p, h, 0, 0))
    return pl.pallas_call(
        functools.partial(fwd_kernel, rows=rows),
        grid=(pages, heads // 2),
        in_specs=[tok, tok, tok, mat],
        out_specs=[mat, tok, tok],
        out_shape=[jax.ShapeDtypeStruct(bias.shape, BF), jax.ShapeDtypeStruct(q.shape, F32), jax.ShapeDtypeStruct(q.shape, F32)],
        name="attn_fwd",
        cost_estimate=pl.CostEstimate(flops=4 * pages * length * length * feat, bytes_accessed=60_000_000, transcendentals=pages * heads * length * length),
    )(q, k, v, bias)


def bwd_kernel(e_ref, q_ref, k_ref, v_ref, do_ref, ctx_ref, dq_ref, dk_ref, dv_ref, ds_ref, *, rows, small_t):
    length = q_ref.shape[0]
    low_half = lax.broadcasted_iota(jnp.int32, (1, 128), 1) < 64
    keys = k_ref[...]
    values = v_ref[...]
    zero = jnp.zeros((), BF)

    def chunk(c, carry):
        at = pl.ds(pl.multiple_of(c * rows, rows), rows)
        do = do_ref[at, :]
        prod = do.astype(F32) * ctx_ref[at, :]
        outs = []
        for j in range(2):
            mine = low_half if j == 0 else jnp.logical_not(low_half)
            delta = jnp.sum(jnp.where(mine, prod, 0.0), axis=1, keepdims=True)
            dp = mm(jnp.where(mine, do, zero), values, NT)
            ds = (e_ref[0, j, at, :].astype(F32) * (dp - delta)).astype(BF)
            ds_ref[0, j, at, :] = ds
            outs.append(mm(ds, keys))
        dq_ref[at, :] = (jnp.where(low_half, outs[0], outs[1]) * 0.125).astype(BF)
        return carry

    lax.fori_loop(0, length // rows, chunk, 0)
    for src, other, dst in ((ds_ref, q_ref, dk_ref), (e_ref, do_ref, dv_ref)):
        if small_t:
            other_t = other[...].T
            top = mm(other_t[:64], src[0, 0])
            bottom = mm(other_t[64:], src[0, 1])
            dst[...] = jnp.concatenate([top, bottom], axis=0).astype(BF).T
        else:
            dst[...] = jnp.where(low_half, mm(src[0, 0], other[...], TN), mm(src[0, 1], other[...], TN)).astype(BF)


def attention_bwd(e, q, k, v, do, ctx, rows=96, small_t=True):
    pages, heads, length, _ = e.shape
    feat = q.shape[1]
    tok = pl.BlockSpec((length, 128), lambda p, h: (p, h))
    mat = pl.BlockSpec((1, 2, length, length), lambda p, h: (p, h, 0, 0))
    return pl.pallas_call(
        functools.partial(bwd_kernel, rows=rows, small_t=small_t),
        grid=(pages, heads // 2),
        in_specs=[mat, tok, tok, tok, tok, tok],
        out_specs=[tok, tok, tok, mat],
        out_shape=[jax.ShapeDtypeStruct(q.shape, BF)] * 3 + [jax.ShapeDtypeStruct(e.shape, BF)],
        name="attn_bwd",
        cost_estimate=pl.CostEstimate(flops=8 * pages * length * length * feat, bytes_accessed=50_000_000, transcendentals=0),
    )(e, q, k, v, do, ctx)


def hist_kernel(near_ref, x_ref, y_ref, ds_ref, out_ref, stage, *, heads, levels):
    group, length = near_ref.shape[1], near_ref.shape[2]
    tiles = -(-length // 128)
    spare = tiles * 128 - length

    @pl.when((pl.program_id(0) == 0) & (pl.program_id(1) == 0))
    def _():
        out_ref[...] = jnp.zeros_like(out_ref)
        for t in range(tiles):
            for r in range(group):
                stage[t, pl.ds(r * 16 + 8, 8), :] = jnp.zeros((8, 128), F32)

    for h in range(heads):
        part = ds_ref[0, h].astype(F32)
        if spare:
            part = jnp.concatenate([part, jnp.zeros((group, spare), F32)], axis=1)
        for t in range(tiles):
            for r in range(0, group, 8):
                stage[t, pl.ds(r * 16 + h, 8, 16), :] = part[r : r + 8, t * 128 : (t + 1) * 128]

    total = jnp.zeros(out_ref.shape, F32)
    for r in range(group):
        marks = []
        for ref, level in zip((near_ref, x_ref, y_ref), levels):
            row = jnp.broadcast_to(ref[0, r : r + 1, :], (level, length))
            marks.append((row == lax.broadcasted_iota(jnp.int32, (level, length), 0)).astype(F32).astype(BF))
        grads = jnp.concatenate([stage[t, pl.ds(r * 16, 16), :].astype(BF) for t in range(tiles)], axis=1)
        total = total + mm(grads[:, :length], jnp.concatenate(marks, axis=0), NT)
    out_ref[...] += total


def table_hist(near, xb, yb, ds, levels, group=16):
    pages, heads, length, _ = ds.shape
    idx = pl.BlockSpec((1, group, length), lambda p, r: (p, r, 0))
    return pl.pallas_call(
        functools.partial(hist_kernel, heads=heads, levels=levels),
        grid=(pages, length // group),
        in_specs=[idx, idx, idx, pl.BlockSpec((1, heads, group, length), lambda p, r: (p, 0, r, 0))],
        out_specs=pl.BlockSpec((16, sum(levels)), lambda p, r: (0, 0)),
        out_shape=jax.ShapeDtypeStruct((16, sum(levels)), F32),
        scratch_shapes=[pltpu.VMEM((-(-length // 128), group * 16, 128), F32)],
        name="hist",
        cost_estimate=pl.CostEstimate(flops=3_000_000_000, bytes_accessed=30_000_000, transcendentals=0),
    )(near, xb, yb, ds)


def gelu_pair(u):
    bell = jnp.exp(-0.5 * u * u)
    phi = 0.5 * (1.0 + lax.erf(u * 0.7071067811865476))
    return u * phi, phi + u * bell * 0.3989422804014327


def norm_parts(rows):
    center = rows - jnp.mean(rows, axis=-1, keepdims=True)
    scale = lax.rsqrt(jnp.mean(center * center, axis=-1, keepdims=True) + 1e-05)
    return center * scale, scale


def norm_back(cot, xhat, scale, gain):
    gc = cot * gain
    return scale * (gc - jnp.mean(gc, axis=-1, keepdims=True) - xhat * jnp.mean(gc * xhat, axis=-1, keepdims=True))


def small_pack(vectors, rows):
    flat = jnp.concatenate([v.reshape(-1) for v in vectors])
    return jnp.pad(flat, (0, rows * 128 - flat.shape[0])).reshape(rows, 128)


AXES = ("dp", "fsdp")


def body(tokens, near, xb, yb, key_mask, out_grad, w_query, w_key, w_value, w_out, w_up, w_down,
         b_query, b_value, b_out, gain_first, shift_first, b_up, b_down, gain_second, shift_second,
         table_near, table_x, table_y):
    micro, pages, length, feat = tokens.shape
    heads = table_near.shape[1]
    own = w_query.shape[0]
    ff = w_up.shape[1]
    count = feat // own
    fsdp = lax.axis_size("fsdp")
    merged = micro * pages
    rows = merged * length
    vectors = (b_query, b_value, b_out, gain_first, shift_first, b_down, gain_second, shift_second, b_up)
    tables = (table_near, table_x, table_y)
    small = small_pack(vectors + tables, own)
    first = lax.all_gather(jnp.concatenate([w_query, w_key, w_value, small], axis=1), AXES, axis=0, tiled=True)
    second = lax.all_gather(jnp.concatenate([w_out, w_up], axis=1), AXES, axis=0, tiled=True)
    w_down_all = lax.all_gather(w_down, AXES, axis=0, tiled=True)
    w_qkv = first[:, : 3 * feat]
    smalls = first[:, 3 * feat :].reshape(count, own * 128)
    at = 0
    full = []
    for v in vectors:
        full.append(smalls[:, at : at + v.shape[0]].reshape(1, -1).astype(F32))
        at += v.shape[0]
    bq, bv, bo, g1, s1, bd, g2, s2, bu = full
    tabs = []
    for which, t in enumerate(tables):
        n = t.shape[0] * fsdp
        full_t = smalls[:fsdp, at : at + t.size].reshape(n, heads).T.astype(F32)
        full_t = jnp.pad(full_t, ((0, 0), (0, 128 - n)))
        if which == 0:
            full_t = full_t.at[:, 127].set(-1e30)
        tabs.append(full_t)
        at += t.size
    levels = tuple(t.shape[0] * fsdp for t in tables)

    near, xb, yb = (a.reshape(merged, length, length) for a in (near, xb, yb))
    mask = key_mask.reshape(merged, 1, length)
    tok = tokens.reshape(rows, feat)
    cot = out_grad.reshape(rows, feat).astype(F32)
    rel_bias = relative_bias(near, xb, yb, mask, jnp.stack(tabs))
    qkv = mm(tok, w_qkv)
    q = (qkv[:, :feat] + bq).astype(BF)
    qs = q * jnp.asarray(0.125, BF)
    k = qkv[:, feat : 2 * feat].astype(BF)
    v = (qkv[:, 2 * feat :] + bv).astype(BF)
    e, ctx, inv = attention_fwd(qs, k, v, rel_bias)
    ctx_low = ctx.astype(BF)
    w_o, w_u = second[:, :feat], second[:, feat:]
    x1, r1 = norm_parts(tok.astype(F32) + (mm(ctx_low, w_o) + bo))
    normed = x1 * g1 + s1
    normed_low = normed.astype(BF)
    hidden, slope = gelu_pair(mm(normed_low, w_u) + bu)
    hidden = hidden.astype(BF)
    slope = slope.astype(BF)
    x2, r2 = norm_parts(normed + (mm(hidden, w_down_all) + bd))
    layer_out = (x2 * g2 + s2).astype(BF)
    d_second = norm_back(cot, x2, r2, g2)
    d_ffn = d_second.astype(BF)
    gw_down = mm(hidden, d_ffn, TN)
    d_pre = (mm(d_ffn, w_down_all, NT) * slope.astype(F32)).astype(BF)
    gw_up = mm(normed_low, d_pre, TN)
    d_normed = d_second + mm(d_pre, w_u, NT)
    d_first = norm_back(d_normed, x1, r1, g1)
    d_attn = d_first.astype(BF)
    gw_out = mm(ctx_low, d_attn, TN)
    d_ctx = (mm(d_attn, w_o, NT) * inv).astype(BF)
    down_share = lax.psum_scatter(gw_down.astype(BF), AXES, scatter_dimension=0, tiled=True)
    up_share = lax.psum_scatter(jnp.concatenate([gw_out.astype(BF), gw_up.astype(BF)], axis=1), AXES, scatter_dimension=0, tiled=True)
    dq, dk, dv, ds = attention_bwd(e, qs, k, v, d_ctx, ctx)
    dqkv = jnp.concatenate([dq, dk, dv], axis=1)
    gw_qkv = mm(tok, dqkv, TN)
    col = lambda a: jnp.sum(a.astype(F32), axis=0)
    parts = (col(dq), col(dv), col(d_attn), col(d_normed * x1), col(d_normed), col(d_ffn), col(cot * x2), col(cot), col(d_pre))
    vec_parts = jnp.concatenate([p.reshape(count, -1) for p in parts], axis=1)
    vec_parts = jnp.pad(vec_parts, ((0, 0), (0, own * 128 - vec_parts.shape[1]))).reshape(feat, 128)
    qkv_share = lax.psum_scatter(jnp.concatenate([gw_qkv, jnp.pad(vec_parts, ((0, 0), (0, 128)))], axis=1).astype(BF), AXES, scatter_dimension=0, tiled=True).astype(F32)
    d_tok = (d_first + mm(dqkv, w_qkv, NT)).astype(BF)
    hist = table_hist(near, xb, yb, ds, levels)[:heads].T
    hist = lax.psum(hist, AXES)
    rank = lax.axis_index("fsdp")
    table_shares = []
    at = 0
    for t, n in zip(tables, levels):
        table_shares.append(lax.dynamic_slice_in_dim(hist, at + rank * t.shape[0], t.shape[0], 0))
        at += n
    vec_share = qkv_share[:, 3 * feat : 3 * feat + 128].reshape(-1)
    vec_out = []
    at = 0
    for v_ in vectors:
        vec_out.append(vec_share[at : at + v_.shape[0]])
        at += v_.shape[0]
    v_bq, v_bv, v_bo, v_g1, v_s1, v_bd, v_g2, v_s2, v_bu = vec_out
    up_share = up_share.astype(F32)
    return (layer_out.reshape(tokens.shape), d_tok.reshape(tokens.shape),
            qkv_share[:, :feat], qkv_share[:, feat : 2 * feat], qkv_share[:, 2 * feat : 3 * feat],
            up_share[:, :feat], up_share[:, feat:], down_share.astype(F32),
            v_bq, v_bv, v_bo, v_g1, v_s1, v_bu, v_bd, v_g2, v_s2, *table_shares)


def solution(mesh):
    pages = P(None, AXES, None, None)
    mat, vec, tab = P(AXES, None), P(AXES), P("fsdp", None)
    return jax.shard_map(
        body,
        mesh=mesh,
        in_specs=(pages,) * 4 + (P(None, AXES, None), pages) + (mat,) * 6 + (vec,) * 9 + (tab,) * 3,
        out_specs=(pages,) * 2 + (mat,) * 6 + (vec,) * 9 + (tab,) * 3,
        check_vma=False,
    )
```

```python
import functools
import jax
import jax.numpy as jnp
from jax import lax
from jax.experimental import pallas as pl
from jax.experimental.pallas import tpu as pltpu
from jax.sharding import PartitionSpec as P

BF, F32 = jnp.bfloat16, jnp.float32
NN = (((1,), (0,)), ((), ()))
NT = (((1,), (1,)), ((), ()))
TN = (((0,), (0,)), ((), ()))


def mm(left, right, dims=NN):
    return lax.dot_general(left, right, dims, preferred_element_type=F32)


MESH_ID = pl.DeviceIdType.MESH


def bits_of(size):
    return [1 << b for b in range(size.bit_length() - 1)]


def flip(position, bit):
    mine = (position // bit) % 2
    return mine, position + (1 - 2 * mine) * bit


def greet(fsdp_size):
    dp, me = lax.axis_index("dp"), lax.axis_index("fsdp")
    barrier = pltpu.get_barrier_semaphore()
    pl.semaphore_signal(barrier, inc=1, device_id=(1 - dp, me), device_id_type=MESH_ID)
    for bit in bits_of(fsdp_size):
        pl.semaphore_signal(barrier, inc=1, device_id=(dp, flip(me, bit)[1]), device_id_type=MESH_ID)
    pl.semaphore_wait(barrier, 1 + len(bits_of(fsdp_size)))


class Gather:
    def __init__(self, size, out, sends, recvs):
        self.size, self.out, self.sends, self.recvs = size, out, sends, recvs
        self.bits = list(reversed(bits_of(size)))
        self.dp, self.me = lax.axis_index("dp"), lax.axis_index("fsdp")
        self.mine = self.dp * size + self.me

    def copies(self, stage):
        base = self.dp * self.size
        if stage == len(self.bits):
            peer = (1 - self.dp, self.me)
            parts = [self.out.at[pl.ds(base, self.size)]]
        else:
            step = 2 * self.bits[stage]
            peer = (self.dp, flip(self.me, self.bits[stage])[1])
            parts = [self.out.at[base + self.me % step + h * step] for h in range(self.size // step)]
        return [
            pltpu.make_async_remote_copy(
                src_ref=part, dst_ref=part, send_sem=self.sends.at[stage, slot],
                recv_sem=self.recvs.at[stage, slot], device_id=peer, device_id_type=MESH_ID)
            for slot, part in enumerate(parts)
        ]

    def start(self, stage):
        for copy in self.copies(stage):
            copy.start()

    def arrive(self, stage):
        for copy in self.copies(stage):
            copy.wait_recv()

    def finish(self):
        for stage in range(len(self.bits) + 1):
            for copy in self.copies(stage):
                copy.wait_send()

    @staticmethod
    def sems(size):
        stages = size.bit_length()
        return [pltpu.SemaphoreType.DMA((stages, size // 2)), pltpu.SemaphoreType.DMA((stages, size // 2))]


class Total:
    def __init__(self, size, sent, landed, sends, recvs):
        self.sent, self.landed, self.sends, self.recvs = sent, landed, sends, recvs
        dp, me = lax.axis_index("dp"), lax.axis_index("fsdp")
        self.peers = [(1 - dp, me)] + [(dp, flip(me, bit)[1]) for bit in bits_of(size)]

    def copy(self, i):
        return pltpu.make_async_remote_copy(
            src_ref=self.sent.at[i], dst_ref=self.landed.at[i], send_sem=self.sends.at[i],
            recv_sem=self.recvs.at[i], device_id=self.peers[i], device_id_type=MESH_ID)

    def arrive(self, i):
        self.copy(i).wait()
        self.sent[i + 1] = self.sent[i] + self.landed[i]

    @staticmethod
    def scratch(size, shape):
        stages = size.bit_length()
        return [pltpu.VMEM((stages + 1, *shape), F32), pltpu.VMEM((stages, *shape), F32),
                pltpu.SemaphoreType.DMA((stages,)), pltpu.SemaphoreType.DMA((stages,))]


class Scatter:
    def __init__(self, size, source, acc, landed, own_sem, sends, recvs):
        self.size, self.source, self.acc, self.landed = size, source, acc, landed
        self.own_sem, self.sends, self.recvs = own_sem, sends, recvs
        self.bits = bits_of(size)
        self.dp, self.me = lax.axis_index("dp"), lax.axis_index("fsdp")

    def place(self, stage):
        return sum(self.size >> s for s in range(stage))

    def own(self):
        return pltpu.make_async_copy(self.source.at[pl.ds(self.dp * self.size, self.size)], self.acc, self.own_sem)

    def copy(self, stage, h):
        if stage == 0:
            part = self.source.at[pl.ds((1 - self.dp) * self.size, self.size)]
            land = self.landed.at[pl.ds(0, self.size)]
            peer = (1 - self.dp, self.me)
        else:
            bit = self.bits[stage - 1]
            mine, other = flip(self.me, bit)
            part = self.acc.at[h * 2 * bit + (1 - mine) * bit + self.me % bit]
            land = self.landed.at[self.place(stage) + h]
            peer = (self.dp, other)
        return pltpu.make_async_remote_copy(
            src_ref=part, dst_ref=land, send_sem=self.sends.at[stage, h], recv_sem=self.recvs.at[stage, h],
            device_id=peer, device_id_type=MESH_ID)

    def count(self, stage):
        return 1 if stage == 0 else self.size >> stage

    def start(self, stage):
        if stage == 0:
            self.own().start()
        for h in range(self.count(stage)):
            self.copy(stage, h).start()

    def arrive(self, stage):
        if stage == 0:
            self.own().wait()
        for h in range(self.count(stage)):
            self.copy(stage, h).wait_recv()
        bit = 0 if stage == 0 else self.bits[stage - 1]
        first = self.place(stage)

        def add(h, carry):
            at = h if stage == 0 else h * 2 * bit + ((self.me // bit) % 2) * bit + self.me % bit
            total = self.acc[at].astype(F32) + self.landed[first + h].astype(F32)
            self.acc[at] = total.astype(self.acc.dtype)
            return carry

        lax.fori_loop(0, self.size >> stage, add, 0)

    def finish(self):
        for stage in range(len(self.bits) + 1):
            for h in range(self.count(stage)):
                self.copy(stage, h).wait_send()

    @staticmethod
    def scratch(size, shape, dtype):
        stages = size.bit_length()
        return [pltpu.VMEM((size, *shape), dtype), pltpu.VMEM((2 * size - 1, *shape), dtype),
                pltpu.SemaphoreType.DMA, pltpu.SemaphoreType.DMA((stages, size // 2)),
                pltpu.SemaphoreType.DMA((stages, size // 2))]


def bias_rows(near_ref, x_ref, y_ref, mask_ref, tab_ref, out_ref, *, heads, length):
    rows = near_ref.shape[1]
    base = pl.program_id(1) * rows

    def group(r, carry):
        start = pl.multiple_of(r * 8, 8)
        for lane in range(0, length, 128):
            width = min(128, length - lane)
            ids = []
            line = base + start + lax.broadcasted_iota(jnp.int32, (8, width), 0)
            column = lane + lax.broadcasted_iota(jnp.int32, (8, width), 1)
            allowed = (mask_ref[0, :, lane : lane + width] > 0) | (line == column)
            for which, ref in enumerate((near_ref, x_ref, y_ref)):
                part = ref[0, pl.ds(start, 8), lane : lane + width]
                if which == 0:
                    part = jnp.where(allowed, part, 127)
                if width < 128:
                    part = jnp.concatenate([part, jnp.zeros((8, 128 - width), jnp.int32)], axis=1)
                ids.append(part)
            sums = [None] * heads
            for which in range(3):
                for h in range(heads):
                    row = jnp.broadcast_to(tab_ref[which, h : h + 1, :], (8, 128))
                    got = jnp.take_along_axis(row, ids[which], axis=1)
                    sums[h] = got if which == 0 else sums[h] + got
            for h in range(heads):
                out_ref[0, h, pl.ds(start, 8), lane : lane + width] = sums[h][:, :width]
        return carry

    lax.fori_loop(0, rows // 8, group, 0)


def bias_specs(near, rows):
    pages, length, _ = near.shape
    idx = pl.BlockSpec((1, rows, length), lambda p, r: (p, r, 0))
    return [idx, idx, idx, pl.BlockSpec((1, 1, length), lambda p, r: (p, 0, 0))]


def bias_out(near, heads, rows):
    pages, length, _ = near.shape
    spec = pl.BlockSpec((1, heads, rows, length), lambda p, r: (p, 0, r, 0))
    return spec, jax.ShapeDtypeStruct((pages, heads, length, length), F32)


BIAS_COST = pl.CostEstimate(flops=30_000_000, bytes_accessed=60_000_000, transcendentals=0)


def relative_bias(near, xb, yb, mask, tabs, rows=96):
    pages, length, _ = near.shape
    heads = tabs.shape[1]
    spec, shape = bias_out(near, heads, rows)
    return pl.pallas_call(
        functools.partial(bias_rows, heads=heads, length=length),
        grid=(pages, length // rows),
        in_specs=bias_specs(near, rows) + [pl.BlockSpec((3, heads, 128), lambda p, r: (0, 0, 0))],
        out_specs=spec,
        out_shape=shape,
        name="bias",
        cost_estimate=BIAS_COST,
    )(near, xb, yb, mask, tabs)


def bias_gather_kernel(near_ref, x_ref, y_ref, mask_ref, wq_ref, wk_ref, wv_ref, *rest, heads, length, size, parts,
                       widths, ticks):
    tables, vectors = rest[: len(parts)], rest[len(parts) : len(parts) + len(widths)]
    (out_ref, whole_ref, smalls_out, smalls_ref, tab_ref, w_own, w_send, w_recv, s_send,
     s_recv) = rest[len(parts) + len(widths) :]
    step = pl.program_id(0) * pl.num_programs(1) + pl.program_id(1)
    last = pl.num_programs(0) * pl.num_programs(1) - 1
    wide = Gather(size, whole_ref, w_send, w_recv)
    small = Gather(size, smalls_ref, s_send, s_recv)
    stages = len(wide.bits)

    @pl.when(step == 0)
    def _():
        copies = []
        for i, ref in enumerate((wq_ref, wk_ref, wv_ref)):
            for p in range(ref.shape[1] // 128):
                copies.append(pltpu.make_async_copy(
                    ref.at[:, p * 128 : (p + 1) * 128],
                    whole_ref.at[wide.mine, :, (3 * p + i) * 128 : (3 * p + i + 1) * 128], w_own.at[i, p]))
                copies[-1].start()
        smalls_ref[small.mine] = jnp.zeros(smalls_ref.shape[1:], F32)
        at = 0
        for ref in (*tables, *vectors):
            smalls_ref[small.mine, at : at + ref.shape[0], : ref.shape[1]] = ref[...].astype(F32)
            at += ref.shape[0]
        greet(size)
        for copy in copies:
            copy.wait()
        small.start(0)
        wide.start(0)
        for stage in range(stages):
            small.arrive(stage)
            small.start(stage + 1)
        lane = lax.broadcasted_iota(jnp.int32, (size, 128), 1)
        owner = lax.broadcasted_iota(jnp.int32, (size, 128), 0)
        base = wide.dp * size
        at = 0
        for which, part in enumerate(parts):
            blocks = [smalls_ref[pl.ds(base, size), at + r, :] for r in range(part)]
            keep = [(lane // part == owner) & (lane % part == r) for r in range(part)]
            for h in range(heads):
                picked = sum(jnp.where(keep[r], blocks[r][:, h : h + 1], 0.0) for r in range(part))
                row = jnp.sum(picked, axis=0, keepdims=True)
                tab_ref[which, h : h + 1, :] = jnp.where(lane[:1] == 127, -1e30, row) if which == 0 else row
            at += part

    for stage, at in enumerate(ticks):
        @pl.when(step == at)
        def _():
            wide.arrive(stage)
            wide.start(stage + 1)

    bias_rows(near_ref, x_ref, y_ref, mask_ref, tab_ref, out_ref, heads=heads, length=length)

    @pl.when(step == last)
    def _():
        small.arrive(stages)
        smalls_out[...] = smalls_ref[...]
        wide.arrive(stages)
        small.finish()
        wide.finish()


def whole_block(array):
    return pl.BlockSpec(array.shape, lambda p, r: (0,) * len(array.shape))


def bias_and_gather(near, xb, yb, mask, weights, tables, vectors, size, rows=96, ticks=(1, 2, 4, 8)):
    pages, length, _ = near.shape
    heads = tables[0].shape[1]
    spec, shape = bias_out(near, heads, rows)
    anywhere = pl.BlockSpec(memory_space=pl.ANY)
    parts = tuple(t.shape[0] for t in tables)
    own, feat = weights[0].shape
    lines = -(-(sum(parts) + len(vectors)) // 8) * 8
    smalls = jax.ShapeDtypeStruct((2 * size, lines, 128), F32)
    return pl.pallas_call(
        functools.partial(bias_gather_kernel, heads=heads, length=length, size=size, parts=parts,
                          widths=tuple(v.shape[1] for v in vectors), ticks=ticks),
        grid=(pages, length // rows),
        in_specs=bias_specs(near, rows) + [anywhere] * 3 + [whole_block(a) for a in (*tables, *vectors)],
        out_specs=[spec, anywhere, whole_block(smalls)],
        out_shape=[shape, jax.ShapeDtypeStruct((2 * size, own, 3 * feat), weights[0].dtype), smalls],
        scratch_shapes=[pltpu.VMEM(smalls.shape, F32), pltpu.VMEM((3, heads, 128), F32),
                        pltpu.SemaphoreType.DMA((3, feat // 128))]
        + Gather.sems(size) + Gather.sems(size),
        name="bias_gather",
        compiler_params=pltpu.CompilerParams(collective_id=1, has_side_effects=True),
        cost_estimate=BIAS_COST,
    )(near, xb, yb, mask, *weights, *tables, *vectors)


def fwd_kernel(q_ref, k_ref, v_ref, bias_ref, e_ref, ctx_ref, low_ref, inv_ref, *, rows):
    length = q_ref.shape[0]
    low_half = lax.broadcasted_iota(jnp.int32, (1, 128), 1) < 64
    keys = k_ref[...]
    values = v_ref[...]
    zero, one = jnp.zeros((), BF), jnp.ones((), BF)
    v_ext = (jnp.where(low_half, values, one), jnp.where(low_half, one, values))

    def chunk(c, carry):
        at = pl.ds(pl.multiple_of(c * rows, rows), rows)
        q = q_ref[at, :]
        q_sel = (jnp.where(low_half, q, zero), jnp.where(low_half, zero, q))
        outs = []
        for j in range(2):
            s = mm(q_sel[j], keys, NT) + bias_ref[0, j, at, :]
            e = jnp.exp(s - jnp.max(s, axis=1, keepdims=True)).astype(BF)
            e_ref[0, j, at, :] = e
            outs.append(mm(e, v_ext[j]))
        total = pltpu.roll(jnp.where(low_half, outs[1], outs[0]), 64, 1)
        inv = 1.0 / total
        inv_ref[at, :] = inv
        context = jnp.where(low_half, outs[0], outs[1]) * inv
        ctx_ref[at, :] = context
        low_ref[at, :] = context.astype(BF)
        return carry

    lax.fori_loop(0, length // rows, chunk, 0)


def pair_specs(length):
    tok = pl.BlockSpec((length, 128), lambda p, h: (p, h))
    mat = pl.BlockSpec((1, 2, length, length), lambda p, h: (p, h, 0, 0))
    qkv = [pl.BlockSpec((length, 128), functools.partial(lambda p, h, i: (p, 3 * h + i), i=i)) for i in range(3)]
    return tok, mat, qkv


def attention_fwd(qkv, bias, rows=96):
    pages, heads, length, _ = bias.shape
    total, feat = qkv.shape[0], qkv.shape[1] // 3
    tok, mat, parts = pair_specs(length)
    like = lambda dtype: jax.ShapeDtypeStruct((total, feat), dtype)
    return pl.pallas_call(
        functools.partial(fwd_kernel, rows=rows),
        grid=(pages, heads // 2),
        in_specs=[*parts, mat],
        out_specs=[mat, tok, tok, tok],
        out_shape=[jax.ShapeDtypeStruct(bias.shape, BF), like(F32), like(BF), like(F32)],
        name="attn_fwd",
        cost_estimate=pl.CostEstimate(flops=4 * pages * length * length * feat, bytes_accessed=60_000_000, transcendentals=pages * heads * length * length),
    )(qkv, qkv, qkv, bias)


def bwd_kernel(e_ref, q_ref, k_ref, v_ref, do_ref, ctx_ref, out_ref, ds_ref, *, rows):
    length = q_ref.shape[0]
    low_half = lax.broadcasted_iota(jnp.int32, (1, 128), 1) < 64
    keys = k_ref[...]
    values = v_ref[...]
    zero = jnp.zeros((), BF)

    def chunk(c, carry):
        at = pl.ds(pl.multiple_of(c * rows, rows), rows)
        do = do_ref[at, :]
        prod = do.astype(F32) * ctx_ref[at, :]
        outs = []
        for j in range(2):
            mine = low_half if j == 0 else jnp.logical_not(low_half)
            delta = jnp.sum(jnp.where(mine, prod, 0.0), axis=1, keepdims=True)
            dp = mm(jnp.where(mine, do, zero), values, NT)
            ds = (e_ref[0, j, at, :].astype(F32) * (dp - delta)).astype(BF)
            ds_ref[0, j, at, :] = ds
            outs.append(mm(ds, keys))
        out_ref[at, :128] = (jnp.where(low_half, outs[0], outs[1]) * 0.125).astype(BF)
        return carry

    lax.fori_loop(0, length // rows, chunk, 0)
    for src, other, lane in ((ds_ref, q_ref, 128), (e_ref, do_ref, 256)):
        other_t = other[...].T
        both = [mm(other_t[:64], src[0, 0]), mm(other_t[64:], src[0, 1])]
        out_ref[:, lane : lane + 128] = jnp.concatenate(both, axis=0).astype(BF).T


def attention_bwd(e, qkv, do, ctx, rows=96):
    pages, heads, length, _ = e.shape
    feat = do.shape[1]
    tok, mat, parts = pair_specs(length)
    return pl.pallas_call(
        functools.partial(bwd_kernel, rows=rows),
        grid=(pages, heads // 2),
        in_specs=[mat, *parts, tok, tok],
        out_specs=[pl.BlockSpec((length, 384), lambda p, h: (p, h)), mat],
        out_shape=[jax.ShapeDtypeStruct(qkv.shape, BF), jax.ShapeDtypeStruct(e.shape, BF)],
        name="attn_bwd",
        cost_estimate=pl.CostEstimate(flops=8 * pages * length * length * feat, bytes_accessed=50_000_000, transcendentals=0),
    )(e, qkv, qkv, qkv, do, ctx)


def hist_rows(near_ref, x_ref, y_ref, ds_ref, out_ref, stage, *, heads, levels):
    group, length = near_ref.shape[1], near_ref.shape[2]
    tiles = -(-length // 128)
    spare = tiles * 128 - length

    @pl.when((pl.program_id(0) == 0) & (pl.program_id(1) == 0))
    def _():
        out_ref[...] = jnp.zeros_like(out_ref)
        for t in range(tiles):
            for r in range(group):
                stage[t, pl.ds(r * 16 + 8, 8), :] = jnp.zeros((8, 128), F32)

    for h in range(heads):
        part = ds_ref[0, h].astype(F32)
        if spare:
            part = jnp.concatenate([part, jnp.zeros((group, spare), F32)], axis=1)
        for t in range(tiles):
            for r in range(0, group, 8):
                stage[t, pl.ds(r * 16 + h, 8, 16), :] = part[r : r + 8, t * 128 : (t + 1) * 128]

    total = jnp.zeros(out_ref.shape, F32)
    for r in range(group):
        marks = []
        for ref, level in zip((near_ref, x_ref, y_ref), levels):
            row = jnp.broadcast_to(ref[0, r : r + 1, :], (level, length))
            marks.append((row == lax.broadcasted_iota(jnp.int32, (level, length), 0)).astype(F32).astype(BF))
        grads = jnp.concatenate([stage[t, pl.ds(r * 16, 16), :].astype(BF) for t in range(tiles)], axis=1)
        total = total + mm(grads[:, :length], jnp.concatenate(marks, axis=0), NT)
    out_ref[...] += total


def hist_specs(ds, group):
    pages, heads, length, _ = ds.shape
    idx = pl.BlockSpec((1, group, length), lambda p, r: (p, r, 0))
    return [idx, idx, idx, pl.BlockSpec((1, heads, group, length), lambda p, r: (p, 0, r, 0))]


def hist_stage(ds, group):
    return pltpu.VMEM((-(-ds.shape[3] // 128), group * 16, 128), F32)


HIST_COST = pl.CostEstimate(flops=3_000_000_000, bytes_accessed=30_000_000, transcendentals=0)


def table_hist(near, xb, yb, ds, levels, group=16):
    pages, heads, length, _ = ds.shape
    return pl.pallas_call(
        functools.partial(hist_rows, heads=heads, levels=levels),
        grid=(pages, length // group),
        in_specs=hist_specs(ds, group),
        out_specs=pl.BlockSpec((16, sum(levels)), lambda p, r: (0, 0)),
        out_shape=jax.ShapeDtypeStruct((16, sum(levels)), F32),
        scratch_shapes=[hist_stage(ds, group)],
        name="hist",
        cost_estimate=HIST_COST,
    )(near, xb, yb, ds)


def own_lanes(row, start, width):
    return pltpu.roll(row, (row.shape[1] - start) % row.shape[1], 1)[:, :width]


def hist_scatter_kernel(near_ref, x_ref, y_ref, ds_ref, wide_ref, plain_ref, qkv_ref, up_ref, *rest, heads, levels, size,
                        parts, ticks):
    vectors, rest = rest[:6], rest[6:]
    (q_out, k_out, v_out, o_out, vec_out, near_out, xt_out, yt_out, stage_ref, total_ref, turned_ref), rest = rest[:11], rest[11:]
    step = pl.program_id(0) * pl.num_programs(1) + pl.program_id(1)
    last = pl.num_programs(0) * pl.num_programs(1) - 1
    hist, vecs = Total(size, *rest[:4]), Total(size, *rest[4:8])
    sums = [Scatter(size, wide_ref, *rest[8:13]), Scatter(size, plain_ref, *rest[13:])]
    me = lax.axis_index("fsdp")
    feat = vectors[0].shape[1]
    pairs = feat // 128

    @pl.when(step == 0)
    def _():
        for which, i in ((0, 0), (1, 2)):
            for p in range(pairs):
                at = (3 * p + i) * 128
                vecs.sent[0, which : which + 1, p * 128 : (p + 1) * 128] = qkv_ref[:, at : at + 128]
        for i, ref in enumerate(vectors):
            vecs.sent[0, 2 + i : 3 + i, :] = ref[...]
        for i in range(up_ref.shape[1] // feat):
            vecs.sent[0, 8 + i : 9 + i, :] = up_ref[:, i * feat : (i + 1) * feat]
        greet(size)
        for s in sums:
            s.start(0)

    for i in range(len(vecs.peers)):
        @pl.when(step == 2 + 4 * i)
        def _():
            vecs.copy(i).start()

        @pl.when(step == 4 + 4 * i)
        def _():
            vecs.arrive(i)

    for stage, at in enumerate(ticks):
        @pl.when(step == at)
        def _():
            for s in sums:
                s.arrive(stage)

        if stage + 1 < len(ticks):
            @pl.when(step == at + 1)
            def _():
                for s in sums:
                    s.start(stage + 1)

    hist_rows(near_ref, x_ref, y_ref, ds_ref, total_ref, stage_ref, heads=heads, levels=levels)

    @pl.when(step == last)
    def _():
        count = len(hist.peers)
        hist.sent[0] = total_ref[...]
        for i, out in enumerate((q_out, k_out, v_out)):
            for p in range(pairs):
                at = (3 * p + i) * 128
                out[:, p * 128 : (p + 1) * 128] = sums[0].acc[me, :, at : at + 128].astype(F32)
        o_out[...] = sums[1].acc[me].astype(F32)
        mine = lax.axis_index("dp") * size + me
        width = feat // (2 * size)
        vec_out[...] = jnp.zeros(vec_out.shape, F32)
        for i in range(8):
            vec_out[i : i + 1, :width] = own_lanes(vecs.sent[count, i : i + 1, :], mine * width, width)
        share = up_ref.shape[1] // (2 * size)
        fold = feat // share
        vec_out[8:9, :share] = own_lanes(vecs.sent[count, pl.ds(8 + mine // fold, 1), :], (mine % fold) * share, share)
        for s in sums:
            s.finish()
        for i in range(count):
            hist.copy(i).start()
            hist.arrive(i)
        full = hist.sent[count]
        spare = -full.shape[1] % 128
        turned_ref[...] = jnp.concatenate([full, jnp.zeros((full.shape[0], spare), F32)], axis=1).T
        at = 0
        for out, part, level in zip((near_out, xt_out, yt_out), parts, levels):
            out[...] = turned_ref[pl.ds(at + me * part, part), :heads]
            at += level


def hist_and_scatter(near, xb, yb, ds, wide, plain, qkv_sum, up_sum, vectors, size, parts, group=16,
                     ticks=(10, 27, 38, 47, 56)):
    pages, heads, length, _ = ds.shape
    levels = tuple(p * size for p in parts)
    anywhere = pl.BlockSpec(memory_space=pl.ANY)
    hist = (16, sum(levels))
    own, feat = plain.shape[1:]
    shape = lambda *dims: jax.ShapeDtypeStruct(dims, F32)
    outs = [shape(own, feat)] * 4 + [shape(16, 128)] + [shape(p, heads) for p in parts]
    return pl.pallas_call(
        functools.partial(hist_scatter_kernel, heads=heads, levels=levels, size=size, parts=parts, ticks=ticks),
        grid=(pages, length // group),
        in_specs=hist_specs(ds, group) + [anywhere, anywhere] + [whole_block(a) for a in (qkv_sum, up_sum, *vectors)],
        out_specs=[whole_block(o) for o in outs],
        out_shape=outs,
        scratch_shapes=[hist_stage(ds, group), pltpu.VMEM(hist, F32), pltpu.VMEM((-(-hist[1] // 128) * 128, 16), F32),
                        *Total.scratch(size, hist), *Total.scratch(size, (16, feat)),
                        *Scatter.scratch(size, wide.shape[1:], wide.dtype),
                        *Scatter.scratch(size, plain.shape[1:], plain.dtype)],
        name="hist_scatter",
        compiler_params=pltpu.CompilerParams(collective_id=2, has_side_effects=True, vmem_limit_bytes=60 << 20),
        cost_estimate=HIST_COST,
    )(near, xb, yb, ds, wide, plain, qkv_sum, up_sum, *vectors)


def gelu_pair(u):
    bell = jnp.exp(-0.5 * u * u)
    phi = 0.5 * (1.0 + lax.erf(u * 0.7071067811865476))
    return u * phi, phi + u * bell * 0.3989422804014327


def norm_parts(rows):
    center = rows - jnp.mean(rows, axis=-1, keepdims=True)
    scale = lax.rsqrt(jnp.mean(center * center, axis=-1, keepdims=True) + 1e-05)
    return center * scale, scale


def norm_back(cot, xhat, scale, gain):
    gc = cot * gain
    return scale * (gc - jnp.mean(gc, axis=-1, keepdims=True) - xhat * jnp.mean(gc * xhat, axis=-1, keepdims=True))


AXES = ("dp", "fsdp")


def by_pair(three, pair=128):
    lead = three[0].shape[:-1]
    split = [a.reshape(*lead, -1, 1, pair) for a in three]
    return jnp.concatenate(split, axis=-2).reshape(*lead, -1)


def from_pair(joined, pair=128):
    lead = joined.shape[:-1]
    split = joined.reshape(*lead, -1, 3, pair)
    return [split[..., i, :].reshape(*lead, -1) for i in range(3)]


def scatter_sum(array):
    return lax.psum_scatter(array, AXES, scatter_dimension=0, tiled=True)


def body(tokens, near, xb, yb, key_mask, out_grad, w_query, w_key, w_value, w_out, w_up, w_down,
         b_query, b_value, b_out, gain_first, shift_first, b_up, b_down, gain_second, shift_second,
         table_near, table_x, table_y):
    micro, pages, length, feat = tokens.shape
    heads = table_near.shape[1]
    own = w_query.shape[0]
    fsdp = lax.axis_size("fsdp")
    count = feat // own
    merged = micro * pages
    rows = merged * length
    vectors = (b_query, b_value, b_out, gain_first, shift_first, b_down, gain_second, shift_second, b_up)
    tables = (table_near, table_x, table_y)
    levels = tuple(t.shape[0] * fsdp for t in tables)
    kernels = own % 8 == 0 and count == 2 * fsdp and fsdp & (fsdp - 1) == 0 and fsdp <= 16

    near, xb, yb = (a.reshape(merged, length, length) for a in (near, xb, yb))
    mask = key_mask.reshape(merged, 1, length)
    tok = tokens.reshape(rows, feat)
    cot = out_grad.reshape(rows, feat).astype(F32)
    second = lax.all_gather(jnp.concatenate([w_out, w_up], axis=1), AXES, axis=0, tiled=True)
    w_down_all = lax.all_gather(w_down, AXES, axis=0, tiled=True)
    if kernels:
        rel_bias, w_qkv, smalls = bias_and_gather(
            near, xb, yb, mask, (w_query, w_key, w_value), tables, [v.reshape(1, -1) for v in vectors], fsdp)
        w_qkv = w_qkv.reshape(feat, 3 * feat)
        first = sum(t.shape[0] for t in tables)
        full = [smalls[:, first + i, : v.shape[0]].reshape(1, -1) for i, v in enumerate(vectors)]
    else:
        w_qkv = lax.all_gather(by_pair((w_query, w_key, w_value)), AXES, axis=0, tiled=True)
        full = [lax.all_gather(v, AXES, axis=0, tiled=True).astype(F32)[None] for v in vectors]
        tabs = []
        for which, t in enumerate(tables):
            full_t = lax.all_gather(t.astype(F32), "fsdp", axis=0, tiled=True).T
            full_t = jnp.pad(full_t, ((0, 0), (0, 128 - full_t.shape[1])))
            tabs.append(full_t.at[:, 127].set(-1e30) if which == 0 else full_t)
        rel_bias = relative_bias(near, xb, yb, mask, jnp.stack(tabs))
    bq, bv, bo, g1, s1, bd, g2, s2, bu = full

    zero = jnp.zeros_like(bq)
    scale = by_pair((zero + 0.125, zero + 1.0, zero + 1.0))
    qkv = ((mm(tok, w_qkv) + by_pair((bq, zero, bv))) * scale).astype(BF)
    e, ctx, ctx_low, inv = attention_fwd(qkv, rel_bias)
    w_o, w_u = second[:, :feat], second[:, feat:]
    x1, r1 = norm_parts(tok.astype(F32) + (mm(ctx_low, w_o) + bo))
    normed = x1 * g1 + s1
    normed_low = normed.astype(BF)
    hidden, slope = gelu_pair(mm(normed_low, w_u) + bu)
    hidden = hidden.astype(BF)
    slope = slope.astype(BF)
    x2, r2 = norm_parts(normed + (mm(hidden, w_down_all) + bd))
    layer_out = (x2 * g2 + s2).astype(BF)
    d_second = norm_back(cot, x2, r2, g2)
    d_ffn = d_second.astype(BF)
    gw_down = mm(hidden, d_ffn, TN).astype(BF)
    d_pre = (mm(d_ffn, w_down_all, NT) * slope.astype(F32)).astype(BF)
    gw_up = mm(normed_low, d_pre, TN).astype(BF)
    d_normed = d_second + mm(d_pre, w_u, NT)
    d_first = norm_back(d_normed, x1, r1, g1)
    d_attn = d_first.astype(BF)
    gw_out = mm(ctx_low, d_attn, TN).astype(BF)
    d_ctx = (mm(d_attn, w_o, NT) * inv).astype(BF)
    down_share = scatter_sum(gw_down)
    up_share = scatter_sum(gw_up)
    d_ctx, _, _ = lax.optimization_barrier((d_ctx, gw_down, gw_up))
    d_qkv, ds = attention_bwd(e, qkv, d_ctx, ctx)
    gw_qkv = mm(tok, d_qkv, TN).astype(BF)
    col = lambda a: jnp.sum(a.astype(F32), axis=0, keepdims=True)
    qkv_sum, up_sum = col(d_qkv), col(d_pre)
    sums = [col(d_attn), col(d_normed * x1), col(d_normed), col(d_ffn), col(cot * x2), col(cot)]
    if kernels:
        gq, gk, gv, go, vec, *table_shares = hist_and_scatter(
            near, xb, yb, ds, gw_qkv.reshape(count, own, 3 * feat), gw_out.reshape(count, own, feat),
            qkv_sum, up_sum, sums, fsdp, tuple(t.shape[0] for t in tables))
        vec_out = [vec[i, :own] for i in range(8)] + [vec[8, : b_up.shape[0]]]
    else:
        gq, gk, gv = from_pair(scatter_sum(gw_qkv).astype(F32))
        go = scatter_sum(gw_out).astype(F32)
        d_bq, _, d_bv = from_pair(qkv_sum)
        vec_out = [scatter_sum(a[0]) for a in (d_bq, d_bv, *sums, up_sum)]
        hist = lax.psum(table_hist(near, xb, yb, ds, levels), AXES)
        table_shares = []
        at = 0
        for t, n in zip(tables, levels):
            share = lax.dynamic_slice_in_dim(hist, at + lax.axis_index("fsdp") * t.shape[0], t.shape[0], 1)
            table_shares.append(share[:heads].T)
            at += n
    d_tok = (d_first + mm(d_qkv, w_qkv, NT)).astype(BF)
    v_bq, v_bv, v_bo, v_g1, v_s1, v_bd, v_g2, v_s2, v_bu = vec_out
    return (layer_out.reshape(tokens.shape), d_tok.reshape(tokens.shape), gq, gk, gv, go,
            up_share.astype(F32), down_share.astype(F32),
            v_bq, v_bv, v_bo, v_g1, v_s1, v_bu, v_bd, v_g2, v_s2, *table_shares)


def solution(mesh):
    pages = P(None, AXES, None, None)
    mat, vec, tab = P(AXES, None), P(AXES), P("fsdp", None)
    return jax.shard_map(
        body,
        mesh=mesh,
        in_specs=(pages,) * 4 + (P(None, AXES, None), pages) + (mat,) * 6 + (vec,) * 9 + (tab,) * 3,
        out_specs=(pages,) * 2 + (mat,) * 6 + (vec,) * 9 + (tab,) * 3,
        check_vma=False,
    )
```
